8 devices in a mesh: dp: 2 (over z, y), tp: 4 (over x, core).
Axes of the slice: x: 2, y: 2, z: 1, core: 2. Of those that a mesh axis runs over, the one named last changes fastest.
Arguments:
- hidden_states: bfloat16 [1024, 4096], P(('dp', 'tp')), parts along dimension 0
- end_pos: int32 [512], P('dp'), parts along dimension 0
- is_final: int32 [512], P('dp'), parts along dimension 0
- norm_gain: float32 [4096], replicated
- w_head: bfloat16 [4096, 32000], P(None, 'tp')
Outputs:
- output 1: float32 [512, 32000], P('dp', 'tp'), parts along dimension 0
- output 2: float32 [512], P('dp'), parts along dimension 0
There are 2 independent parts. The reference program is written for one: setup_inputs(seed, part) draws one part's arguments, and reference() takes and returns one part's arrays. A program takes and returns all parts, laid end to end along the dimension named above; an argument that names none is the same for every part.
All inputs are finite; a program needn't handle non-finite values.
Results may differ from the reference program's by a relative error of at most 0.001.
Values are sent between devices in bfloat16 or wider.
A program may use at most 1 GiB of HBM per device.

```python
import jax
import jax.numpy as jnp
from jax import lax

HIDDEN = 4096
VOCAB_SIZE = 32000
TOK_DEV = 128
REQUESTS = 256
GROUP_SIZE = 4
TOKENS = TOK_DEV * GROUP_SIZE
NORM_EPS = 1e-5
HEAD_SCALE = 3.0


def draw_end_positions(key):
    key_rank, key_off, key_noise = jax.random.split(key, 3)
    block_rank = jax.random.permutation(key_rank, GROUP_SIZE)
    positions = jnp.arange(TOKENS, dtype=jnp.int32)
    owner = positions // TOK_DEV
    pos_rank = block_rank[owner]
    offsets = jax.random.randint(key_off, (GROUP_SIZE,), 0, TOK_DEV)
    forced = ((positions % TOK_DEV == offsets[owner]) & (pos_rank < 3)) | (positions == TOKENS - 1)
    noise = jax.random.randint(key_noise, (TOKENS,), 0, 1024)
    priority = jnp.where(forced, -1, jnp.where(pos_rank < 3, 0, 1024) + noise)
    score = priority * TOKENS + positions
    chosen = lax.top_k(-score, REQUESTS)[1]
    return jnp.sort(chosen).astype(jnp.int32)


def draw_flags(key):
    flags = jax.random.randint(key, (REQUESTS,), 0, 2).astype(jnp.int32)
    return flags.at[0].set(1).at[1].set(0)


def setup_inputs(seed: int = 0, part: int = 0) -> dict:
    key_gain, key_head = jax.random.split(jax.random.key(seed), 2)
    part_key = jax.random.fold_in(jax.random.key(seed + 1), part)
    key_hidden, key_pos, key_flag = jax.random.split(part_key, 3)
    hidden_states = jax.random.normal(key_hidden, (TOKENS, HIDDEN), jnp.float32).astype(jnp.bfloat16)
    norm_gain = jax.random.uniform(key_gain, (HIDDEN,), jnp.float32, 0.5, 1.5)
    w_head = (jax.random.normal(key_head, (HIDDEN, VOCAB_SIZE), jnp.float32) * (HEAD_SCALE * HIDDEN ** -0.5)).astype(jnp.bfloat16)
    return {"hidden_states": hidden_states, "end_pos": draw_end_positions(key_pos), "is_final": draw_flags(key_flag), "norm_gain": norm_gain, "w_head": w_head}


def reference(hidden_states, end_pos, is_final, norm_gain, w_head):
    sel_rows = jnp.take(hidden_states, end_pos, axis=0).astype(jnp.float32)
    inv_rms = lax.rsqrt(jnp.mean(sel_rows * sel_rows, axis=1, keepdims=True) + NORM_EPS)
    normed = (sel_rows * inv_rms * norm_gain[None, :]).astype(jnp.bfloat16)
    logits = jnp.dot(normed, w_head, preferred_element_type=jnp.float32)
    log_norm = jax.nn.logsumexp(logits, axis=1)
    log_probs = jnp.where(is_final[:, None] == 1, logits - log_norm[:, None], 0.0)
    return (log_probs, log_norm)
```

```python
import functools

import jax
import jax.numpy as jnp
from jax import lax
from jax.experimental import pallas as pl
from jax.experimental.pallas import tpu as pltpu
from jax.sharding import PartitionSpec as P

NORM_EPS = 1e-5
MESH = pl.DeviceIdType.MESH
CW = 256
WK = 512
W_SLOTS = 5
W_PIECES = 4
ROWS_OUT = 1000


def gather_head_kernel(
    hidden_ref, pos_ref, gain_ref, w_ref, logits_ref, norm_ref,
    rows, w_ring, onehot, x_buf, inv_buf, stat_buf,
    own_sem, w_sem, xs_sem, xr_sem, ps_sem, pr_sem, fs_sem, fr_sem, is_sem, ir_sem, ss_sem, sr_sem,
):
    n_tok, hidden = hidden_ref.shape
    vocab = w_ref.shape[0]
    n_req = pos_ref.shape[1]
    n_slices = hidden // CW
    n_w = hidden // WK
    per_w = WK // CW
    dp, me = lax.axis_index("dp"), lax.axis_index("tp")
    across = lax.rem(me + 2, 4)
    partner = me + 1 - 2 * lax.rem(me, 2)
    corner = lax.rem(partner + 2, 4)
    peers = (across, partner, corner)

    def block(owner):
        return pl.ds(pl.multiple_of(owner * n_tok, n_tok), n_tok)

    def own_copy(j):
        return pltpu.make_async_copy(
            hidden_ref.at[:, pl.ds(j * CW, CW)], rows.at[j, block(me)], own_sem.at[j]
        )

    def w_copy(s, p):
        m = vocab // W_PIECES
        return pltpu.make_async_copy(
            w_ref.at[pl.ds(p * m, m), pl.ds(s * WK, WK)],
            w_ring.at[s % W_SLOTS, pl.ds(p * m, m)],
            w_sem.at[s % W_SLOTS, p],
        )

    def send_rows(j, owner, send, recv, target):
        return pltpu.make_async_remote_copy(
            src_ref=rows.at[j, block(owner)], dst_ref=rows.at[j, block(owner)],
            send_sem=send.at[j], recv_sem=recv.at[j],
            device_id=(dp, target), device_id_type=MESH,
        )

    def to_across(j):
        return send_rows(j, me, xs_sem, xr_sem, across)

    def to_partner(j):
        return send_rows(j, me, ps_sem, pr_sem, partner)

    def forward(j):
        return send_rows(j, across, fs_sem, fr_sem, partner)

    def send_small(buf, i, send, recv):
        return pltpu.make_async_remote_copy(
            src_ref=buf.at[me], dst_ref=buf.at[me], send_sem=send.at[i], recv_sem=recv.at[i],
            device_id=(dp, peers[i]), device_id_type=MESH,
        )

    for j in range(n_slices):
        own_copy(j).start()
    for s in range(min(W_SLOTS, n_w)):
        for p in range(W_PIECES):
            w_copy(s, p).start()

    barrier = pltpu.get_barrier_semaphore()
    for peer in peers:
        pl.semaphore_signal(barrier, inc=1, device_id=(dp, peer), device_id_type=MESH)
    pl.semaphore_wait(barrier, 3)

    early = 3
    for j in range(early):
        own_copy(j).wait()
        to_across(j).start()
        to_partner(j).start()
    for j in range(early, n_slices):
        own_copy(j).wait()
        to_partner(j).start()
    total = jnp.zeros((n_tok, CW), jnp.float32)
    for j in range(n_slices):
        r = rows[j, block(me)].astype(jnp.float32)
        total += r * r
    inv = lax.rsqrt(jnp.sum(total, axis=1, keepdims=True) * (1.0 / hidden) + NORM_EPS)
    eye = lax.broadcasted_iota(jnp.int32, (n_tok, n_tok), 0) == lax.broadcasted_iota(jnp.int32, (n_tok, n_tok), 1)
    inv_row = jnp.sum(jnp.where(eye, inv, 0.0), axis=0, keepdims=True)
    inv_buf[me] = jnp.broadcast_to(inv_row, inv_buf.shape[1:])
    picks = lax.broadcasted_iota(jnp.int32, (4 * n_tok, n_req), 0) == pos_ref[...]
    onehot[...] = jnp.where(picks, 1.0, 0.0).T.astype(jnp.bfloat16)
    for i in range(3):
        send_small(inv_buf, i, is_sem, ir_sem).start()
    for j in range(early, n_slices):
        to_across(j).start()

    for i in range(3):
        send_small(inv_buf, i, is_sem, ir_sem).wait_recv()
    inv_sel = jnp.zeros((n_req, 1), jnp.float32)
    for o in range(4):
        hit = onehot[:, o * n_tok:(o + 1) * n_tok].astype(jnp.float32)
        inv_sel += jnp.sum(hit * inv_buf[o, 0:1, :], axis=1, keepdims=True)

    def prepare(j, k):
        to_partner(j).wait_recv()
        forward(j).wait_recv()
        r = jnp.dot(onehot[...], rows[j], preferred_element_type=jnp.float32)
        x_buf[:, k * CW:(k + 1) * CW] = (r * inv_sel * gain_ref[:, j * CW:(j + 1) * CW]).astype(jnp.bfloat16)

    def relay(j):
        to_across(j).wait_recv()
        forward(j).start()

    steps = [tuple(range(s * per_w, (s + 1) * per_w)) for s in range(n_w - 1)]
    steps += [(j,) for j in range((n_w - 1) * per_w, n_w * per_w)]
    mb = vocab // 2
    for j in steps[0]:
        relay(j)
    run_max = jnp.full((1, n_req), -jnp.inf, jnp.float32)
    run_sum = jnp.zeros((1, n_req), jnp.float32)
    for i, cols in enumerate(steps):
        if i + 1 < len(steps):
            for j in steps[i + 1]:
                relay(j)
        for k, j in enumerate(cols):
            prepare(j, k)
        s, width = cols[0] // per_w, len(cols) * CW
        off = (cols[0] % per_w) * CW
        if off == 0:
            for p in range(W_PIECES):
                w_copy(s, p).wait()
        first, last = i == 0, i + 1 == len(steps)

        def body(m, carry):
            at = pl.ds(pl.multiple_of(m * mb, 8), mb)
            z = lax.dot_general(
                w_ring[s % W_SLOTS, at, off:off + width], x_buf[:, :width],
                (((1,), (1,)), ((), ())), preferred_element_type=jnp.float32,
            )
            if not first:
                z += logits_ref[at, :]
            logits_ref[at, :] = z
            return carry

        lax.fori_loop(0, vocab // mb, body, 0)
        if off + width == WK and s + W_SLOTS < n_w:
            for p in range(W_PIECES):
                w_copy(s + W_SLOTS, p).start()

    sb = ROWS_OUT

    def stat_body(m, carry):
        run_max, run_sum = carry
        z = logits_ref[pl.ds(pl.multiple_of(m * sb, 8), sb), :]
        new_max = jnp.maximum(run_max, jnp.max(z, axis=0, keepdims=True))
        run_sum = run_sum * jnp.exp(run_max - new_max) + jnp.sum(jnp.exp(z - new_max), axis=0, keepdims=True)
        return new_max, run_sum

    run_max, run_sum = lax.fori_loop(0, vocab // sb, stat_body, (run_max, run_sum))
    stat_buf[me, 0:1, :] = run_max
    stat_buf[me, 1:2, :] = run_sum
    for i in range(3):
        send_small(stat_buf, i, ss_sem, sr_sem).start()
    for j in range(n_slices):
        to_across(j).wait_send()
        to_partner(j).wait_send()
        forward(j).wait_send()
    for i in range(3):
        send_small(inv_buf, i, is_sem, ir_sem).wait_send()
    for i in range(3):
        send_small(stat_buf, i, ss_sem, sr_sem).wait()
    group_max = jnp.max(stat_buf[:, 0, :], axis=0, keepdims=True)
    group_sum = jnp.sum(stat_buf[:, 1, :] * jnp.exp(stat_buf[:, 0, :] - group_max), axis=0, keepdims=True)
    norm_ref[...] = group_max + jnp.log(group_sum)


def finish_kernel(logits_ref, norm_ref, flag_ref, out_ref, norm_out_ref, stage, sem):
    vocab = logits_ref.shape[0]
    n = vocab // ROWS_OUT
    keep = flag_ref[...] == 1
    norm = norm_ref[...]
    norm_out_ref[...] = norm

    def out_copy(m):
        at = pl.ds(m * ROWS_OUT, ROWS_OUT)
        return pltpu.make_async_copy(stage.at[at], out_ref.at[at], sem.at[m])

    for m in range(n):
        at = pl.ds(m * ROWS_OUT, ROWS_OUT)
        stage[at, :] = jnp.where(keep, logits_ref[at, :] - norm, 0.0)
        out_copy(m).start()
    for m in range(n):
        out_copy(m).wait()


def solution(mesh):
    def body(hidden_blk, end_pos, is_final, norm_gain, w_block):
        n_tok, hidden = hidden_blk.shape
        vocab = w_block.shape[1]
        n_req = end_pos.shape[0]
        n_slices = hidden // CW
        f32 = jnp.float32
        vmem = pl.BlockSpec(memory_space=pltpu.VMEM)
        hbm = pl.BlockSpec(memory_space=pl.ANY)
        dma = pltpu.SemaphoreType.DMA
        logits, norm = pl.pallas_call(
            gather_head_kernel,
            out_shape=(pltpu.VMEM((vocab, n_req), f32), pltpu.VMEM((1, n_req), f32)),
            in_specs=[hbm, vmem, vmem, hbm],
            out_specs=(vmem, vmem),
            scratch_shapes=[
                pltpu.VMEM((n_slices, 4 * n_tok, CW), jnp.bfloat16),
                pltpu.VMEM((W_SLOTS, vocab, WK), jnp.bfloat16),
                pltpu.VMEM((n_req, 4 * n_tok), jnp.bfloat16),
                pltpu.VMEM((n_req, WK), jnp.bfloat16),
                pltpu.VMEM((4, 8, n_tok), f32),
                pltpu.VMEM((4, 8, n_req), f32),
                dma((n_slices,)), dma((W_SLOTS, W_PIECES)),
                dma((n_slices,)), dma((n_slices,)), dma((n_slices,)), dma((n_slices,)),
                dma((n_slices,)), dma((n_slices,)), dma((3,)), dma((3,)), dma((3,)), dma((3,)),
            ],
            compiler_params=pltpu.CompilerParams(
                collective_id=0, has_side_effects=True, vmem_limit_bytes=54 * 1024 * 1024
            ),
            name="gather_head",
        )(hidden_blk, end_pos.reshape(1, n_req), norm_gain.reshape(1, hidden), w_block.T)
        out, log_norm = pl.pallas_call(
            finish_kernel,
            out_shape=(jax.ShapeDtypeStruct((vocab, n_req), f32), jax.ShapeDtypeStruct((1, n_req), f32)),
            in_specs=[vmem, vmem, vmem],
            out_specs=(hbm, vmem),
            scratch_shapes=[pltpu.VMEM((vocab, n_req), f32), dma((vocab // ROWS_OUT,))],
            compiler_params=pltpu.CompilerParams(vmem_limit_bytes=20 * 1024 * 1024),
            name="finish",
        )(logits, norm, is_final.reshape(1, n_req))
        return out.T, log_norm.reshape(n_req)

    return jax.shard_map(
        body,
        mesh=mesh,
        in_specs=(P(("dp", "tp"), None), P("dp"), P("dp"), P(None), P(None, "tp")),
        out_specs=(P("dp", "tp"), P("dp")),
        check_vma=False,
    )
```

```python
import functools

import jax
import jax.numpy as jnp
from jax import lax
from jax.experimental import pallas as pl
from jax.experimental.pallas import tpu as pltpu
from jax.sharding import PartitionSpec as P

NORM_EPS = 1e-5
MESH = pl.DeviceIdType.MESH
CW = 256
WK = 512
W_SLOTS = 5
W_PIECES = 4
ROWS_OUT = 1000


def gather_head_kernel(
    hidden_ref, pos_ref, gain_ref, w_ref, logits_ref, norm_ref,
    rows, w_ring, onehot, x_buf, inv_buf, stat_buf,
    own_sem, w_sem, xs_sem, xr_sem, ps_sem, pr_sem, fs_sem, fr_sem, is_sem, ir_sem, ss_sem, sr_sem,
):
    n_tok, hidden = hidden_ref.shape
    vocab = w_ref.shape[0]
    n_req = pos_ref.shape[1]
    n_slices = hidden // CW
    n_w = hidden // WK
    per_w = WK // CW
    dp, me = lax.axis_index("dp"), lax.axis_index("tp")
    across = lax.rem(me + 2, 4)
    partner = me + 1 - 2 * lax.rem(me, 2)
    corner = lax.rem(partner + 2, 4)
    peers = (across, partner, corner)

    def block(owner):
        return pl.ds(pl.multiple_of(owner * n_tok, n_tok), n_tok)

    def own_copy(j):
        return pltpu.make_async_copy(
            hidden_ref.at[:, pl.ds(j * CW, CW)], rows.at[j, block(me)], own_sem.at[j]
        )

    def w_copy(s, p):
        m = vocab // W_PIECES
        return pltpu.make_async_copy(
            w_ref.at[pl.ds(p * m, m), pl.ds(s * WK, WK)],
            w_ring.at[s % W_SLOTS, pl.ds(p * m, m)],
            w_sem.at[s % W_SLOTS, p],
        )

    def send_rows(j, owner, send, recv, target):
        return pltpu.make_async_remote_copy(
            src_ref=rows.at[j, block(owner)], dst_ref=rows.at[j, block(owner)],
            send_sem=send.at[j], recv_sem=recv.at[j],
            device_id=(dp, target), device_id_type=MESH,
        )

    def to_across(j):
        return send_rows(j, me, xs_sem, xr_sem, across)

    def to_partner(j):
        return send_rows(j, me, ps_sem, pr_sem, partner)

    def forward(j):
        return send_rows(j, across, fs_sem, fr_sem, partner)

    def send_small(buf, i, send, recv):
        return pltpu.make_async_remote_copy(
            src_ref=buf.at[me], dst_ref=buf.at[me], send_sem=send.at[i], recv_sem=recv.at[i],
            device_id=(dp, peers[i]), device_id_type=MESH,
        )

    for j in range(n_slices):
        own_copy(j).start()
    for s in range(min(W_SLOTS, n_w)):
        for p in range(W_PIECES):
            w_copy(s, p).start(priority=1)

    barrier = pltpu.get_barrier_semaphore()
    for peer in peers:
        pl.semaphore_signal(barrier, inc=1, device_id=(dp, peer), device_id_type=MESH)
    pl.semaphore_wait(barrier, 3)

    early = 3
    for j in range(early):
        own_copy(j).wait()
        to_across(j).start()
        to_partner(j).start()
    for j in range(early, n_slices):
        own_copy(j).wait()
        to_partner(j).start()
    total = jnp.zeros((n_tok, CW), jnp.float32)
    for j in range(n_slices):
        r = rows[j, block(me)].astype(jnp.float32)
        total += r * r
    inv = lax.rsqrt(jnp.sum(total, axis=1, keepdims=True) * (1.0 / hidden) + NORM_EPS)
    eye = lax.broadcasted_iota(jnp.int32, (n_tok, n_tok), 0) == lax.broadcasted_iota(jnp.int32, (n_tok, n_tok), 1)
    inv_row = jnp.sum(jnp.where(eye, inv, 0.0), axis=0, keepdims=True)
    inv_buf[me] = jnp.broadcast_to(inv_row, inv_buf.shape[1:])
    picks = lax.broadcasted_iota(jnp.int32, (4 * n_tok, n_req), 0) == pos_ref[...]
    onehot[...] = jnp.where(picks, 1.0, 0.0).T.astype(jnp.bfloat16)
    for i in range(3):
        send_small(inv_buf, i, is_sem, ir_sem).start()
    for j in range(early, n_slices):
        to_across(j).start()

    for i in range(3):
        send_small(inv_buf, i, is_sem, ir_sem).wait_recv()
    inv_sel = jnp.zeros((n_req, 1), jnp.float32)
    for o in range(4):
        hit = onehot[:, o * n_tok:(o + 1) * n_tok].astype(jnp.float32)
        inv_sel += jnp.sum(hit * inv_buf[o, 0:1, :], axis=1, keepdims=True)

    def prepare(j, k):
        to_partner(j).wait_recv()
        forward(j).wait_recv()
        r = jnp.dot(onehot[...], rows[j], preferred_element_type=jnp.float32)
        x_buf[:, k * CW:(k + 1) * CW] = (r * inv_sel * gain_ref[:, j * CW:(j + 1) * CW]).astype(jnp.bfloat16)

    def relay(j):
        to_across(j).wait_recv()
        forward(j).start()

    steps = [tuple(range(s * per_w, (s + 1) * per_w)) for s in range(n_w - 1)]
    steps += [(j,) for j in range((n_w - 1) * per_w, n_w * per_w)]
    mb = vocab // 2
    for j in steps[0]:
        relay(j)
    run_max = jnp.full((1, n_req), -jnp.inf, jnp.float32)
    run_sum = jnp.zeros((1, n_req), jnp.float32)
    for i, cols in enumerate(steps):
        if i + 1 < len(steps):
            for j in steps[i + 1]:
                relay(j)
        for k, j in enumerate(cols):
            prepare(j, k)
        s, width = cols[0] // per_w, len(cols) * CW
        off = (cols[0] % per_w) * CW
        if off == 0:
            for p in range(W_PIECES):
                w_copy(s, p).wait()
        first, last = i == 0, i + 1 == len(steps)

        def body(m, carry):
            at = pl.ds(pl.multiple_of(m * mb, 8), mb)
            z = lax.dot_general(
                w_ring[s % W_SLOTS, at, off:off + width], x_buf[:, :width],
                (((1,), (1,)), ((), ())), preferred_element_type=jnp.float32,
            )
            if not first:
                z += logits_ref[at, :]
            logits_ref[at, :] = z
            return carry

        lax.fori_loop(0, vocab // mb, body, 0)
        if off + width == WK and s + W_SLOTS < n_w:
            for p in range(W_PIECES):
                w_copy(s + W_SLOTS, p).start(priority=1)

    sb = ROWS_OUT

    def stat_body(m, carry):
        run_max, run_sum = carry
        z = logits_ref[pl.ds(pl.multiple_of(m * sb, 8), sb), :]
        new_max = jnp.maximum(run_max, jnp.max(z, axis=0, keepdims=True))
        run_sum = run_sum * jnp.exp(run_max - new_max) + jnp.sum(jnp.exp(z - new_max), axis=0, keepdims=True)
        return new_max, run_sum

    run_max, run_sum = lax.fori_loop(0, vocab // sb, stat_body, (run_max, run_sum))
    stat_buf[me, 0:1, :] = run_max
    stat_buf[me, 1:2, :] = run_sum
    for i in range(3):
        send_small(stat_buf, i, ss_sem, sr_sem).start()
    for j in range(n_slices):
        to_across(j).wait_send()
        to_partner(j).wait_send()
        forward(j).wait_send()
    for i in range(3):
        send_small(inv_buf, i, is_sem, ir_sem).wait_send()
    for i in range(3):
        send_small(stat_buf, i, ss_sem, sr_sem).wait()
    group_max = jnp.max(stat_buf[:, 0, :], axis=0, keepdims=True)
    group_sum = jnp.sum(stat_buf[:, 1, :] * jnp.exp(stat_buf[:, 0, :] - group_max), axis=0, keepdims=True)
    norm_ref[...] = group_max + jnp.log(group_sum)


def finish_kernel(logits_ref, norm_ref, flag_ref, out_ref, norm_out_ref, stage, sem):
    vocab = logits_ref.shape[0]
    n = vocab // ROWS_OUT
    keep = flag_ref[...] == 1
    norm = norm_ref[...]
    norm_out_ref[...] = norm

    def out_copy(m):
        at = pl.ds(m * ROWS_OUT, ROWS_OUT)
        return pltpu.make_async_copy(stage.at[at], out_ref.at[at], sem.at[m])

    for m in range(n):
        at = pl.ds(m * ROWS_OUT, ROWS_OUT)
        stage[at, :] = jnp.where(keep, logits_ref[at, :] - norm, 0.0)
        out_copy(m).start()
    for m in range(n):
        out_copy(m).wait()


def solution(mesh):
    def body(hidden_blk, end_pos, is_final, norm_gain, w_block):
        n_tok, hidden = hidden_blk.shape
        vocab = w_block.shape[1]
        n_req = end_pos.shape[0]
        n_slices = hidden // CW
        f32 = jnp.float32
        vmem = pl.BlockSpec(memory_space=pltpu.VMEM)
        hbm = pl.BlockSpec(memory_space=pl.ANY)
        dma = pltpu.SemaphoreType.DMA
        logits, norm = pl.pallas_call(
            gather_head_kernel,
            out_shape=(pltpu.VMEM((vocab, n_req), f32), pltpu.VMEM((1, n_req), f32)),
            in_specs=[hbm, vmem, vmem, hbm],
            out_specs=(vmem, vmem),
            scratch_shapes=[
                pltpu.VMEM((n_slices, 4 * n_tok, CW), jnp.bfloat16),
                pltpu.VMEM((W_SLOTS, vocab, WK), jnp.bfloat16),
                pltpu.VMEM((n_req, 4 * n_tok), jnp.bfloat16),
                pltpu.VMEM((n_req, WK), jnp.bfloat16),
                pltpu.VMEM((4, 8, n_tok), f32),
                pltpu.VMEM((4, 8, n_req), f32),
                dma((n_slices,)), dma((W_SLOTS, W_PIECES)),
                dma((n_slices,)), dma((n_slices,)), dma((n_slices,)), dma((n_slices,)),
                dma((n_slices,)), dma((n_slices,)), dma((3,)), dma((3,)), dma((3,)), dma((3,)),
            ],
            compiler_params=pltpu.CompilerParams(
                collective_id=0, has_side_effects=True, vmem_limit_bytes=54 * 1024 * 1024
            ),
            name="gather_head",
        )(hidden_blk, end_pos.reshape(1, n_req), norm_gain.reshape(1, hidden), w_block.T)
        out, log_norm = pl.pallas_call(
            finish_kernel,
            out_shape=(jax.ShapeDtypeStruct((vocab, n_req), f32), jax.ShapeDtypeStruct((1, n_req), f32)),
            in_specs=[vmem, vmem, vmem],
            out_specs=(hbm, vmem),
            scratch_shapes=[pltpu.VMEM((vocab, n_req), f32), dma((vocab // ROWS_OUT,))],
            compiler_params=pltpu.CompilerParams(vmem_limit_bytes=20 * 1024 * 1024),
            name="finish",
        )(logits, norm, is_final.reshape(1, n_req))
        return out.T, log_norm.reshape(n_req)

    return jax.shard_map(
        body,
        mesh=mesh,
        in_specs=(P(("dp", "tp"), None), P("dp"), P("dp"), P(None), P(None, "tp")),
        out_specs=(P("dp", "tp"), P("dp")),
        check_vma=False,
    )
```

```python
import functools

import jax
import jax.numpy as jnp
from jax import lax
from jax.experimental import pallas as pl
from jax.experimental.pallas import tpu as pltpu
from jax.sharding import PartitionSpec as P

NORM_EPS = 1e-5
MESH = pl.DeviceIdType.MESH
CW = 256
WK = 512
W_SLOTS = 5
W_PIECES = 4
ROWS_OUT = 1000
CUTS = {2: (3200, 6400), 1: (3200, 4800)}
EDGES = (0, 2400, 4800, 6400, 7360, 8000)
SPLITS = {-1: (1, 1)}


def gather_head_kernel(
    hidden_ref, pos_hbm, gain_hbm, w_ref, logits_ref, norm_ref,
    rows, w_ring, onehot, x_buf, inv_buf, stat_buf, pos_ref, gain_ref,
    own_sem, w_sem, in_sem, xs_sem, xr_sem, ps_sem, pr_sem, fs_sem, fr_sem, is_sem, ir_sem, ss_sem, sr_sem,
):
    n_tok, hidden = hidden_ref.shape
    vocab = w_ref.shape[0]
    n_req = pos_ref.shape[1]
    n_slices = hidden // CW
    n_w = hidden // WK
    per_w = WK // CW
    dp, me = lax.axis_index("dp"), lax.axis_index("tp")
    across = lax.rem(me + 2, 4)
    partner = me + 1 - 2 * lax.rem(me, 2)
    corner = lax.rem(partner + 2, 4)
    peers = (across, partner, corner)

    barrier = pltpu.get_barrier_semaphore()
    for peer in peers:
        pl.semaphore_signal(barrier, inc=1, device_id=(dp, peer), device_id_type=MESH)

    def block(owner):
        return pl.ds(pl.multiple_of(owner * n_tok, n_tok), n_tok)

    def own_copy(j):
        return pltpu.make_async_copy(
            hidden_ref.at[:, pl.ds(j * CW, CW)], rows.at[j, block(me)], own_sem.at[j]
        )

    def w_copy(s, p):
        m = vocab // W_PIECES
        return pltpu.make_async_copy(
            w_ref.at[pl.ds(p * m, m), pl.ds(s * WK, WK)],
            w_ring.at[s % W_SLOTS, pl.ds(p * m, m)],
            w_sem.at[s % W_SLOTS, p],
        )

    def send_rows(j, owner, send, recv, target):
        return pltpu.make_async_remote_copy(
            src_ref=rows.at[j, block(owner)], dst_ref=rows.at[j, block(owner)],
            send_sem=send.at[j], recv_sem=recv.at[j],
            device_id=(dp, target), device_id_type=MESH,
        )

    def to_across(j):
        return send_rows(j, me, xs_sem, xr_sem, across)

    def to_partner(j):
        return send_rows(j, me, ps_sem, pr_sem, partner)

    def forward(j):
        return send_rows(j, across, fs_sem, fr_sem, partner)

    def send_small(buf, i, send, recv):
        return pltpu.make_async_remote_copy(
            src_ref=buf.at[me], dst_ref=buf.at[me], send_sem=send.at[i], recv_sem=recv.at[i],
            device_id=(dp, peers[i]), device_id_type=MESH,
        )

    small = (
        pltpu.make_async_copy(pos_hbm, pos_ref, in_sem.at[0]),
        pltpu.make_async_copy(gain_hbm, gain_ref, in_sem.at[1]),
    )
    for j in range(n_slices):
        own_copy(j).start()
    for copy in small:
        copy.start()
    for s in range(min(W_SLOTS, n_w)):
        for p in range(W_PIECES):
            w_copy(s, p).start(priority=1)
    pl.semaphore_wait(barrier, 3)

    early = 2
    for j in range(early):
        own_copy(j).wait()
        to_across(j).start()
        to_partner(j).start()
    for j in range(early, n_slices):
        own_copy(j).wait()
        to_partner(j).start()
    total = jnp.zeros((n_tok, CW), jnp.float32)
    for j in range(n_slices):
        r = rows[j, block(me)].astype(jnp.float32)
        total += r * r
    inv = lax.rsqrt(jnp.sum(total, axis=1, keepdims=True) * (1.0 / hidden) + NORM_EPS)
    eye = lax.broadcasted_iota(jnp.int32, (n_tok, n_tok), 0) == lax.broadcasted_iota(jnp.int32, (n_tok, n_tok), 1)
    inv_row = jnp.sum(jnp.where(eye, inv, 0.0), axis=0, keepdims=True)
    inv_buf[me] = jnp.broadcast_to(inv_row, inv_buf.shape[1:])
    for copy in small:
        copy.wait()
    picks = lax.broadcasted_iota(jnp.int32, (4 * n_tok, n_req), 0) == pos_ref[...]
    onehot[...] = jnp.where(picks, 1.0, 0.0).T.astype(jnp.bfloat16)
    for i in range(3):
        send_small(inv_buf, i, is_sem, ir_sem).start()
    for j in range(early, n_slices):
        to_across(j).start()

    for i in range(3):
        send_small(inv_buf, i, is_sem, ir_sem).wait_recv()
    inv_sel = jnp.zeros((n_req, 1), jnp.float32)
    for o in range(4):
        hit = onehot[:, o * n_tok:(o + 1) * n_tok].astype(jnp.float32)
        inv_sel += jnp.sum(hit * inv_buf[o, 0:1, :], axis=1, keepdims=True)

    def relay(j):
        to_across(j).wait_recv()
        forward(j).start()

    def arrived(j):
        to_partner(j).wait_recv()
        forward(j).wait_recv()

    def prepare(j, k, slot):
        r = jnp.dot(onehot[...], rows[j], preferred_element_type=jnp.float32)
        x = r * inv_sel * gain_ref[:, j * CW:(j + 1) * CW]
        x_buf[slot, :, k * CW:(k + 1) * CW] = x.astype(jnp.bfloat16)

    steps = []
    for s in range(n_w):
        for width in SPLITS.get(s - n_w, SPLITS.get(s, (per_w,))):
            first = steps[-1][-1] + 1 if steps else 0
            steps.append(tuple(range(first, first + width)))

    once = 1 + me // 4

    def alone(work, *carry):
        return lax.fori_loop(0, once, lambda k, c: work(*c), carry)

    def multiply(i, start, size):
        cols = steps[i]
        off, width = cols[0] % per_w * CW, len(cols) * CW
        z = lax.dot_general(
            w_ring[cols[0] // per_w % W_SLOTS, start:start + size, off:off + width], x_buf[i % 2, :, :width],
            (((1,), (1,)), ((), ())), preferred_element_type=jnp.float32,
        )
        if i > 0:
            z += logits_ref[start:start + size, :]
        logits_ref[start:start + size, :] = z
        return z

    def piece(i, start, stop, extra=None):
        if start == stop:
            return

        def work():
            if extra is not None:
                extra()
            multiply(i, start, stop - start)
            return ()

        alone(work)

    lanes = 4 * 8

    def highest(z, run_max):
        return jnp.maximum(run_max, jnp.max(z.reshape(z.shape[0] // lanes, lanes, n_req), axis=0))

    def add_up(start, stop, run_max, ref, run_sum):
        z = logits_ref[start:stop, :].reshape((stop - start) // lanes, lanes, n_req)
        return run_sum * jnp.exp(ref - run_max) + jnp.sum(jnp.exp(z - run_max), axis=0)

    def w_wait(s):
        for p in range(W_PIECES):
            w_copy(s, p).wait()

    last = len(steps) - 1
    for j in steps[0]:
        relay(j)
    for k, j in enumerate(steps[0]):
        arrived(j)
        prepare(j, k, 0)
    w_wait(0)
    pending = [j for cols in steps[1:] for j in cols]
    for i in range(last):
        cols, nxt = steps[i], steps[i + 1]
        cut_1, cut_2 = CUTS[len(cols)]
        piece(i, 0, cut_1)
        for j in nxt:
            if j in pending:
                relay(j)
                pending.remove(j)
        piece(i, cut_1, cut_2)
        if len(nxt) == 1 and i + 2 <= last:
            for j in steps[i + 2]:
                relay(j)
                pending.remove(j)
        for j in nxt:
            arrived(j)

        def prepare_next():
            for k, j in enumerate(nxt):
                prepare(j, k, (i + 1) % 2)

        piece(i, cut_2, vocab, prepare_next)
        s = cols[0] // per_w
        if nxt[0] // per_w != s:
            if s + W_SLOTS < n_w:
                for p in range(W_PIECES):
                    w_copy(s + W_SLOTS, p).start(priority=1)
            w_wait(s + 1)
    low = jnp.full((lanes, n_req), -jnp.inf, jnp.float32)
    run_max, = alone(lambda m: (highest(multiply(last, EDGES[0], EDGES[1]), m),), low)
    ref, run_sum = run_max, jnp.zeros((lanes, n_req), jnp.float32)
    for k in range(1, len(EDGES) - 1):
        def final(run_max, ref, run_sum):
            z = multiply(last, EDGES[k], EDGES[k + 1] - EDGES[k])
            run_sum = add_up(EDGES[k - 1], EDGES[k], run_max, ref, run_sum)
            return highest(z, run_max), run_max, run_sum

        run_max, ref, run_sum = alone(final, run_max, ref, run_sum)
    run_sum = add_up(EDGES[-2], EDGES[-1], run_max, ref, run_sum)
    local_max = jnp.max(run_max, axis=0, keepdims=True)
    stat_buf[me, 0:1, :] = local_max
    stat_buf[me, 1:2, :] = jnp.sum(run_sum * jnp.exp(run_max - local_max), axis=0, keepdims=True)
    for i in range(3):
        send_small(stat_buf, i, ss_sem, sr_sem).start()
    for j in range(n_slices):
        to_across(j).wait_send()
        to_partner(j).wait_send()
        forward(j).wait_send()
    for i in range(3):
        send_small(inv_buf, i, is_sem, ir_sem).wait_send()
    for i in range(3):
        send_small(stat_buf, i, ss_sem, sr_sem).wait()
    group_max = jnp.max(stat_buf[:, 0, :], axis=0, keepdims=True)
    group_sum = jnp.sum(stat_buf[:, 1, :] * jnp.exp(stat_buf[:, 0, :] - group_max), axis=0, keepdims=True)
    norm_ref[...] = group_max + jnp.log(group_sum)


def finish_kernel(logits_ref, norm_ref, flag_ref, out_ref, norm_out_ref, stage, sem):
    vocab = logits_ref.shape[0]
    n = vocab // ROWS_OUT
    keep = flag_ref[...] == 1
    norm = norm_ref[...]
    norm_out_ref[...] = norm

    def out_copy(m):
        at = pl.ds(m * ROWS_OUT, ROWS_OUT)
        return pltpu.make_async_copy(stage.at[at], out_ref.at[at], sem.at[m])

    for m in range(n):
        at = pl.ds(m * ROWS_OUT, ROWS_OUT)
        stage[at, :] = jnp.where(keep, logits_ref[at, :] - norm, 0.0)
        out_copy(m).start()
    for m in range(n):
        out_copy(m).wait()


def solution(mesh):
    def body(hidden_blk, end_pos, is_final, norm_gain, w_block):
        n_tok, hidden = hidden_blk.shape
        vocab = w_block.shape[1]
        n_req = end_pos.shape[0]
        n_slices = hidden // CW
        f32 = jnp.float32
        vmem = pl.BlockSpec(memory_space=pltpu.VMEM)
        hbm = pl.BlockSpec(memory_space=pl.ANY)
        dma = pltpu.SemaphoreType.DMA
        logits, norm = pl.pallas_call(
            gather_head_kernel,
            out_shape=(pltpu.VMEM((vocab, n_req), f32), pltpu.VMEM((1, n_req), f32)),
            in_specs=[hbm, hbm, hbm, hbm],
            out_specs=(vmem, vmem),
            scratch_shapes=[
                pltpu.VMEM((n_slices, 4 * n_tok, CW), jnp.bfloat16),
                pltpu.VMEM((W_SLOTS, vocab, WK), jnp.bfloat16),
                pltpu.VMEM((n_req, 4 * n_tok), jnp.bfloat16),
                pltpu.VMEM((2, n_req, WK), jnp.bfloat16),
                pltpu.VMEM((4, 8, n_tok), f32),
                pltpu.VMEM((4, 8, n_req), f32),
                pltpu.VMEM((1, n_req), jnp.int32),
                pltpu.VMEM((1, hidden), f32),
                dma((n_slices,)), dma((W_SLOTS, W_PIECES)), dma((2,)),
                dma((n_slices,)), dma((n_slices,)), dma((n_slices,)), dma((n_slices,)),
                dma((n_slices,)), dma((n_slices,)), dma((3,)), dma((3,)), dma((3,)), dma((3,)),
            ],
            compiler_params=pltpu.CompilerParams(
                collective_id=0, has_side_effects=True, vmem_limit_bytes=54 * 1024 * 1024
            ),
            name="gather_head",
        )(hidden_blk, end_pos.reshape(1, n_req), norm_gain.reshape(1, hidden), w_block.T)
        out, log_norm = pl.pallas_call(
            finish_kernel,
            out_shape=(jax.ShapeDtypeStruct((vocab, n_req), f32), jax.ShapeDtypeStruct((1, n_req), f32)),
            in_specs=[vmem, vmem, vmem],
            out_specs=(hbm, vmem),
            scratch_shapes=[pltpu.VMEM((vocab, n_req), f32), dma((vocab // ROWS_OUT,))],
            compiler_params=pltpu.CompilerParams(vmem_limit_bytes=20 * 1024 * 1024),
            name="finish",
        )(logits, norm, is_final.reshape(1, n_req))
        return out.T, log_norm.reshape(n_req)

    return jax.shard_map(
        body,
        mesh=mesh,
        in_specs=(P(("dp", "tp"), None), P("dp"), P("dp"), P(None), P(None, "tp")),
        out_specs=(P("dp", "tp"), P("dp")),
        check_vma=False,
    )
```

```python
import jax
import jax.numpy as jnp
from jax import lax
from jax.experimental import pallas as pl
from jax.experimental.pallas import tpu as pltpu
from jax.sharding import PartitionSpec as P

NORM_EPS = 1e-5
MESH = pl.DeviceIdType.MESH
CW = 256
WK = 512
W_SLOTS = 5
W_PIECES = 4
ROWS_OUT = 1000
LAST = 800


def gather_head_kernel(
    hidden_ref, pos_hbm, gain_hbm, w_ref, logits_ref, norm_ref,
    rows, w_ring, onehot, x_buf, inv_buf, stat_buf, pos_ref, gain_ref,
    own_sem, w_sem, in_sem, xs_sem, xr_sem, ps_sem, pr_sem, fs_sem, fr_sem, is_sem, ir_sem, ss_sem, sr_sem,
):
    n_tok, hidden = hidden_ref.shape
    vocab = w_ref.shape[0]
    n_req = pos_ref.shape[1]
    n_slices = hidden // CW
    n_w = hidden // WK
    per_w = WK // CW
    dp, me = lax.axis_index("dp"), lax.axis_index("tp")
    across = lax.rem(me + 2, 4)
    partner = me + 1 - 2 * lax.rem(me, 2)
    corner = lax.rem(partner + 2, 4)
    peers = (across, partner, corner)

    barrier = pltpu.get_barrier_semaphore()
    for peer in peers:
        pl.semaphore_signal(barrier, inc=1, device_id=(dp, peer), device_id_type=MESH)

    def block(owner):
        return pl.ds(pl.multiple_of(owner * n_tok, n_tok), n_tok)

    def own_copy(j):
        return pltpu.make_async_copy(
            hidden_ref.at[:, pl.ds(j * CW, CW)], rows.at[j, block(me)], own_sem.at[j]
        )

    def w_copy(s, p):
        m = vocab // W_PIECES
        return pltpu.make_async_copy(
            w_ref.at[pl.ds(p * m, m), pl.ds(s * WK, WK)],
            w_ring.at[s % W_SLOTS, pl.ds(p * m, m)],
            w_sem.at[s % W_SLOTS, p],
        )

    def send_rows(j, owner, send, recv, target):
        return pltpu.make_async_remote_copy(
            src_ref=rows.at[j, block(owner)], dst_ref=rows.at[j, block(owner)],
            send_sem=send.at[j], recv_sem=recv.at[j],
            device_id=(dp, target), device_id_type=MESH,
        )

    def to_across(j):
        return send_rows(j, me, xs_sem, xr_sem, across)

    def to_partner(j):
        return send_rows(j, me, ps_sem, pr_sem, partner)

    def forward(j):
        return send_rows(j, across, fs_sem, fr_sem, partner)

    def send_small(buf, i, send, recv):
        return pltpu.make_async_remote_copy(
            src_ref=buf.at[me], dst_ref=buf.at[me], send_sem=send.at[i], recv_sem=recv.at[i],
            device_id=(dp, peers[i]), device_id_type=MESH,
        )

    small = (
        pltpu.make_async_copy(pos_hbm, pos_ref, in_sem.at[0]),
        pltpu.make_async_copy(gain_hbm, gain_ref, in_sem.at[1]),
    )
    for j in range(n_slices):
        own_copy(j).start()
    for copy in small:
        copy.start()
    for s in range(min(W_SLOTS, n_w)):
        for p in range(W_PIECES):
            w_copy(s, p).start(priority=1)
    pl.semaphore_wait(barrier, 3)

    own_copy(0).wait()
    to_across(0).start()
    to_partner(0).start()
    for j in range(1, n_slices):
        own_copy(j).wait()
    total = jnp.zeros((n_tok, CW), jnp.float32)
    for j in range(n_slices):
        r = rows[j, block(me)].astype(jnp.float32)
        total += r * r
    inv = lax.rsqrt(jnp.sum(total, axis=1, keepdims=True) * (1.0 / hidden) + NORM_EPS)
    eye = lax.broadcasted_iota(jnp.int32, (n_tok, n_tok), 0) == lax.broadcasted_iota(jnp.int32, (n_tok, n_tok), 1)
    inv_row = jnp.sum(jnp.where(eye, inv, 0.0), axis=0, keepdims=True)
    inv_buf[me] = jnp.broadcast_to(inv_row, inv_buf.shape[1:])
    for j in range(1, n_slices):
        to_partner(j).start()
    for i in range(3):
        send_small(inv_buf, i, is_sem, ir_sem).start()
    for j in range(1, n_slices):
        to_across(j).start()
    for copy in small:
        copy.wait()
    picks = lax.broadcasted_iota(jnp.int32, (4 * n_tok, n_req), 0) == pos_ref[...]
    onehot[...] = jnp.where(picks, 1.0, 0.0).T.astype(jnp.bfloat16)

    def relay(j):
        to_across(j).wait_recv()
        forward(j).start()

    relay(0)
    for i in range(3):
        send_small(inv_buf, i, is_sem, ir_sem).wait_recv()
    inv_sel = jnp.zeros((n_req, 1), jnp.float32)
    for o in range(4):
        hit = onehot[:, o * n_tok:(o + 1) * n_tok].astype(jnp.float32)
        inv_sel += jnp.sum(hit * inv_buf[o, 0:1, :], axis=1, keepdims=True)

    def arrived(j):
        to_partner(j).wait_recv()
        forward(j).wait_recv()

    def prepare(j, k, slot):
        r = jnp.dot(onehot[...], rows[j], preferred_element_type=jnp.float32)
        x = r * inv_sel * gain_ref[:, j * CW:(j + 1) * CW]
        x_buf[slot, :, k * CW:(k + 1) * CW] = x.astype(jnp.bfloat16)

    steps = [tuple(range(s * per_w, (s + 1) * per_w)) for s in range(n_w)]
    once = 1 + me // 4

    def alone(work, *carry):
        return lax.fori_loop(0, once, lambda k, c: work(*c), carry)

    def multiply(i, start, size, lo=0, hi=WK):
        at = pl.ds(start, size)
        z = lax.dot_general(
            w_ring[i % W_SLOTS, at, lo:hi], x_buf[i % 2, :, lo:hi],
            (((1,), (1,)), ((), ())), preferred_element_type=jnp.float32,
        )
        if i > 0 or lo > 0:
            z += logits_ref[at, :]
        logits_ref[at, :] = z
        return z

    lanes = 4 * 8

    def highest(z, run_max):
        return jnp.maximum(run_max, jnp.max(z.reshape(z.shape[0] // lanes, lanes, n_req), axis=0))

    def w_wait(s):
        for p in range(W_PIECES):
            w_copy(s, p).wait()

    last = len(steps) - 1
    mid = vocab // 2
    def first_rows(i):
        prepare(steps[i][1], 1, i % 2)
        multiply(i, 0, mid, 0, CW)
        return multiply(i, 0, mid, CW, WK)

    def other_rows(i):
        prepare(steps[i + 1][0], 0, (i + 1) % 2)
        multiply(i, mid, vocab - mid)

    arrived(0)
    prepare(0, 0, 0)
    relay(1)
    w_wait(0)
    for i in range(last):
        nxt = steps[i + 1]
        arrived(steps[i][1])
        relay(nxt[0])
        alone(lambda: (first_rows(i), ())[1])
        relay(nxt[1])
        arrived(nxt[0])
        alone(lambda: (other_rows(i), ())[1])
        if i + W_SLOTS < n_w:
            for p in range(W_PIECES):
                w_copy(i + W_SLOTS, p).start(priority=1)
        w_wait(i + 1)
    arrived(steps[last][1])
    run_max = jnp.full((lanes, n_req), -jnp.inf, jnp.float32)
    ref, = alone(lambda m: (highest(first_rows(last), m),), run_max)

    def add_up(k, run_sum, top):
        z = logits_ref[pl.ds(pl.multiple_of(k * LAST, lanes), LAST), :]
        return run_sum + jnp.sum(jnp.exp(z.reshape(LAST // lanes, lanes, n_req) - top), axis=0)

    def second(ref):
        run_max = highest(multiply(last, mid, vocab - mid), ref)
        run_sum = jnp.zeros((lanes, n_req), jnp.float32)
        for k in range(mid // LAST):
            run_sum = add_up(k, run_sum, ref)
        return run_max, run_sum * jnp.exp(ref - run_max)

    run_max, run_sum = lax.fori_loop(0, once, lambda k, c: second(ref), (run_max, run_max))
    run_sum = lax.fori_loop(mid // LAST, vocab // LAST, lambda k, c: add_up(k, c, run_max), run_sum)
    local_max = jnp.max(run_max, axis=0, keepdims=True)
    stat_buf[me, 0:1, :] = local_max
    stat_buf[me, 1:2, :] = jnp.sum(run_sum * jnp.exp(run_max - local_max), axis=0, keepdims=True)
    for i in range(3):
        send_small(stat_buf, i, ss_sem, sr_sem).start()
    for j in range(n_slices):
        to_across(j).wait_send()
        to_partner(j).wait_send()
        forward(j).wait_send()
    for i in range(3):
        send_small(inv_buf, i, is_sem, ir_sem).wait_send()
    for i in range(3):
        send_small(stat_buf, i, ss_sem, sr_sem).wait()
    group_max = jnp.max(stat_buf[:, 0, :], axis=0, keepdims=True)
    group_sum = jnp.sum(stat_buf[:, 1, :] * jnp.exp(stat_buf[:, 0, :] - group_max), axis=0, keepdims=True)
    norm_ref[...] = group_max + jnp.log(group_sum)


def finish_kernel(logits_ref, norm_ref, flag_ref, out_ref, norm_out_ref, stage, sem):
    vocab = logits_ref.shape[0]
    n = vocab // ROWS_OUT
    keep = flag_ref[...] == 1
    norm = norm_ref[...]
    norm_out_ref[...] = norm

    def out_copy(m):
        at = pl.ds(m * ROWS_OUT, ROWS_OUT)
        return pltpu.make_async_copy(stage.at[at], out_ref.at[at], sem.at[m])

    for m in range(n):
        at = pl.ds(m * ROWS_OUT, ROWS_OUT)
        stage[at, :] = jnp.where(keep, logits_ref[at, :] - norm, 0.0)
        out_copy(m).start()
    for m in range(n):
        out_copy(m).wait()


def solution(mesh):
    def body(hidden_blk, end_pos, is_final, norm_gain, w_block):
        n_tok, hidden = hidden_blk.shape
        vocab = w_block.shape[1]
        n_req = end_pos.shape[0]
        n_slices = hidden // CW
        f32 = jnp.float32
        vmem = pl.BlockSpec(memory_space=pltpu.VMEM)
        hbm = pl.BlockSpec(memory_space=pl.ANY)
        dma = pltpu.SemaphoreType.DMA
        logits, norm = pl.pallas_call(
            gather_head_kernel,
            out_shape=(pltpu.VMEM((vocab, n_req), f32), pltpu.VMEM((1, n_req), f32)),
            in_specs=[hbm, hbm, hbm, hbm],
            out_specs=(vmem, vmem),
            scratch_shapes=[
                pltpu.VMEM((n_slices, 4 * n_tok, CW), jnp.bfloat16),
                pltpu.VMEM((W_SLOTS, vocab, WK), jnp.bfloat16),
                pltpu.VMEM((n_req, 4 * n_tok), jnp.bfloat16),
                pltpu.VMEM((2, n_req, WK), jnp.bfloat16),
                pltpu.VMEM((4, 8, n_tok), f32),
                pltpu.VMEM((4, 8, n_req), f32),
                pltpu.VMEM((1, n_req), jnp.int32),
                pltpu.VMEM((1, hidden), f32),
                dma((n_slices,)), dma((W_SLOTS, W_PIECES)), dma((2,)),
                dma((n_slices,)), dma((n_slices,)), dma((n_slices,)), dma((n_slices,)),
                dma((n_slices,)), dma((n_slices,)), dma((3,)), dma((3,)), dma((3,)), dma((3,)),
            ],
            compiler_params=pltpu.CompilerParams(
                collective_id=0, has_side_effects=True, vmem_limit_bytes=54 * 1024 * 1024
            ),
            name="gather_head",
        )(hidden_blk, end_pos.reshape(1, n_req), norm_gain.reshape(1, hidden), w_block.T)
        out, log_norm = pl.pallas_call(
            finish_kernel,
            out_shape=(jax.ShapeDtypeStruct((vocab, n_req), f32), jax.ShapeDtypeStruct((1, n_req), f32)),
            in_specs=[vmem, vmem, vmem],
            out_specs=(hbm, vmem),
            scratch_shapes=[pltpu.VMEM((vocab, n_req), f32), dma((vocab // ROWS_OUT,))],
            compiler_params=pltpu.CompilerParams(vmem_limit_bytes=20 * 1024 * 1024),
            name="finish",
        )(logits, norm, is_final.reshape(1, n_req))
        return out.T, log_norm.reshape(n_req)

    return jax.shard_map(
        body,
        mesh=mesh,
        in_specs=(P(("dp", "tp"), None), P("dp"), P("dp"), P(None), P(None, "tp")),
        out_specs=(P("dp", "tp"), P("dp")),
        check_vma=False,
    )
```

```python
import jax
import jax.numpy as jnp
from jax import lax
from jax.experimental import pallas as pl
from jax.experimental.pallas import tpu as pltpu
from jax.sharding import PartitionSpec as P

NORM_EPS = 1e-5
MESH = pl.DeviceIdType.MESH
CW = 256
WK = 512
W_SLOTS = 5
W_PIECES = 4
ROWS_OUT = 1000
FIRST = 5600
LAST = 800


def gather_head_kernel(
    hidden_ref, pos_hbm, gain_hbm, w_ref, logits_ref, norm_ref,
    rows, w_ring, onehot, x_buf, inv_buf, stat_buf, pos_ref, gain_ref,
    own_sem, w_sem, in_sem, xs_sem, xr_sem, ps_sem, pr_sem, fs_sem, fr_sem, is_sem, ir_sem, ss_sem, sr_sem,
):
    n_tok, hidden = hidden_ref.shape
    vocab = w_ref.shape[0]
    n_req = pos_ref.shape[1]
    n_slices = hidden // CW
    n_w = hidden // WK
    per_w = WK // CW
    dp, me = lax.axis_index("dp"), lax.axis_index("tp")
    across = lax.rem(me + 2, 4)
    partner = me + 1 - 2 * lax.rem(me, 2)
    corner = lax.rem(partner + 2, 4)
    peers = (across, partner, corner)

    barrier = pltpu.get_barrier_semaphore()
    for peer in peers:
        pl.semaphore_signal(barrier, inc=1, device_id=(dp, peer), device_id_type=MESH)

    def block(owner):
        return pl.ds(pl.multiple_of(owner * n_tok, n_tok), n_tok)

    def own_copy(j):
        return pltpu.make_async_copy(
            hidden_ref.at[:, pl.ds(j * CW, CW)], rows.at[j, block(me)], own_sem.at[j]
        )

    def w_copy(s, p):
        m = vocab // W_PIECES
        return pltpu.make_async_copy(
            w_ref.at[pl.ds(p * m, m), pl.ds(s * WK, WK)],
            w_ring.at[s % W_SLOTS, pl.ds(p * m, m)],
            w_sem.at[s % W_SLOTS, p],
        )

    def send_rows(j, owner, send, recv, target):
        return pltpu.make_async_remote_copy(
            src_ref=rows.at[j, block(owner)], dst_ref=rows.at[j, block(owner)],
            send_sem=send.at[j], recv_sem=recv.at[j],
            device_id=(dp, target), device_id_type=MESH,
        )

    def to_across(j):
        return send_rows(j, me, xs_sem, xr_sem, across)

    def to_partner(j):
        return send_rows(j, me, ps_sem, pr_sem, partner)

    def forward(j):
        return send_rows(j, across, fs_sem, fr_sem, partner)

    def send_small(buf, i, send, recv):
        return pltpu.make_async_remote_copy(
            src_ref=buf.at[me], dst_ref=buf.at[me], send_sem=send.at[i], recv_sem=recv.at[i],
            device_id=(dp, peers[i]), device_id_type=MESH,
        )

    small = (
        pltpu.make_async_copy(pos_hbm, pos_ref, in_sem.at[0]),
        pltpu.make_async_copy(gain_hbm, gain_ref, in_sem.at[1]),
    )
    for j in range(n_slices):
        own_copy(j).start()
    for copy in small:
        copy.start()
    for s in range(min(W_SLOTS, n_w)):
        for p in range(W_PIECES):
            w_copy(s, p).start(priority=1)
    pl.semaphore_wait(barrier, 3)

    own_copy(0).wait()
    to_across(0).start()
    to_partner(0).start()
    for j in range(1, n_slices):
        own_copy(j).wait()
    total = jnp.zeros((n_tok, CW), jnp.float32)
    for j in range(n_slices):
        r = rows[j, block(me)].astype(jnp.float32)
        total += r * r
    inv = lax.rsqrt(jnp.sum(total, axis=1, keepdims=True) * (1.0 / hidden) + NORM_EPS)
    eye = lax.broadcasted_iota(jnp.int32, (n_tok, n_tok), 0) == lax.broadcasted_iota(jnp.int32, (n_tok, n_tok), 1)
    inv_row = jnp.sum(jnp.where(eye, inv, 0.0), axis=0, keepdims=True)
    inv_buf[me] = jnp.broadcast_to(inv_row, inv_buf.shape[1:])
    for j in range(1, n_slices):
        to_partner(j).start()
    for i in range(3):
        send_small(inv_buf, i, is_sem, ir_sem).start()
    for j in range(1, n_slices):
        to_across(j).start()
    for copy in small:
        copy.wait()
    picks = lax.broadcasted_iota(jnp.int32, (4 * n_tok, n_req), 0) == pos_ref[...]
    onehot[...] = jnp.where(picks, 1.0, 0.0).T.astype(jnp.bfloat16)

    def relay(j):
        to_across(j).wait_recv()
        forward(j).start()

    relay(0)
    for i in range(3):
        send_small(inv_buf, i, is_sem, ir_sem).wait_recv()
    inv_sel = jnp.zeros((n_req, 1), jnp.float32)
    for o in range(4):
        hit = onehot[:, o * n_tok:(o + 1) * n_tok].astype(jnp.float32)
        inv_sel += jnp.sum(hit * inv_buf[o, 0:1, :], axis=1, keepdims=True)

    def arrived(j):
        to_partner(j).wait_recv()
        forward(j).wait_recv()

    def prepare(j, k, slot):
        r = jnp.dot(onehot[...], rows[j], preferred_element_type=jnp.float32)
        x = r * inv_sel * gain_ref[:, j * CW:(j + 1) * CW]
        x_buf[slot, :, k * CW:(k + 1) * CW] = x.astype(jnp.bfloat16)

    steps = [tuple(range(s * per_w, (s + 1) * per_w)) for s in range(n_w)]
    once = 1 + me // 4

    def alone(work, *carry):
        return lax.fori_loop(0, once, lambda k, c: work(*c), carry)

    def multiply(i, start, size, lo=0, hi=WK):
        at = pl.ds(start, size)
        z = lax.dot_general(
            w_ring[i % W_SLOTS, at, lo:hi], x_buf[i % 2, :, lo:hi],
            (((1,), (1,)), ((), ())), preferred_element_type=jnp.float32,
        )
        if i > 0 or lo > 0:
            z += logits_ref[at, :]
        logits_ref[at, :] = z
        return z

    lanes = 4 * 8

    def highest(z, run_max):
        return jnp.maximum(run_max, jnp.max(z.reshape(z.shape[0] // lanes, lanes, n_req), axis=0))

    def w_wait(s):
        for p in range(W_PIECES):
            w_copy(s, p).wait()

    last = len(steps) - 1
    mid = vocab // 2

    def first_rows(i, mid=mid):
        prepare(steps[i][1], 1, i % 2)
        multiply(i, 0, mid, 0, CW)
        return multiply(i, 0, mid, CW, WK)

    def other_rows(i):
        prepare(steps[i + 1][0], 0, (i + 1) % 2)
        multiply(i, mid, vocab - mid)

    arrived(0)
    prepare(0, 0, 0)
    relay(1)
    w_wait(0)
    for i in range(last):
        nxt = steps[i + 1]
        arrived(steps[i][1])
        relay(nxt[0])
        alone(lambda: (first_rows(i), ())[1])
        relay(nxt[1])
        arrived(nxt[0])
        alone(lambda: (other_rows(i), ())[1])
        if i + W_SLOTS < n_w:
            for p in range(W_PIECES):
                w_copy(i + W_SLOTS, p).start(priority=1)
        w_wait(i + 1)
    arrived(steps[last][1])
    run_max = jnp.full((lanes, n_req), -jnp.inf, jnp.float32)

    def add_up(k, run_sum, top):
        z = logits_ref[pl.ds(pl.multiple_of(k * LAST, lanes), LAST), :]
        return run_sum + jnp.sum(jnp.exp(z.reshape(LAST // lanes, lanes, n_req) - top), axis=0)

    def second(ref):
        ref = highest(first_rows(last, FIRST), ref)
        run_max = highest(multiply(last, FIRST, vocab - FIRST), ref)
        run_sum = jnp.zeros((lanes, n_req), jnp.float32)
        for k in range(FIRST // LAST):
            run_sum = add_up(k, run_sum, ref)
        return run_max, run_sum * jnp.exp(ref - run_max)

    run_max, run_sum = lax.fori_loop(0, once, lambda k, c: second(c[0]), (run_max, run_max))
    run_sum = lax.fori_loop(FIRST // LAST, vocab // LAST, lambda k, c: add_up(k, c, run_max), run_sum)
    local_max = jnp.max(run_max, axis=0, keepdims=True)
    stat_buf[me, 0:1, :] = local_max
    stat_buf[me, 1:2, :] = jnp.sum(run_sum * jnp.exp(run_max - local_max), axis=0, keepdims=True)
    for i in range(3):
        send_small(stat_buf, i, ss_sem, sr_sem).start()
    for j in range(n_slices):
        to_across(j).wait_send()
        to_partner(j).wait_send()
        forward(j).wait_send()
    for i in range(3):
        send_small(inv_buf, i, is_sem, ir_sem).wait_send()
    for i in range(3):
        send_small(stat_buf, i, ss_sem, sr_sem).wait()
    group_max = jnp.max(stat_buf[:, 0, :], axis=0, keepdims=True)
    group_sum = jnp.sum(stat_buf[:, 1, :] * jnp.exp(stat_buf[:, 0, :] - group_max), axis=0, keepdims=True)
    norm_ref[...] = group_max + jnp.log(group_sum)


def finish_kernel(logits_ref, norm_ref, flag_ref, out_ref, norm_out_ref, stage, sem, norm_sem):
    vocab = logits_ref.shape[0]
    n = vocab // ROWS_OUT
    keep = flag_ref[...] == 1
    norm = norm_ref[...]
    norm_copy = pltpu.make_async_copy(norm_ref, norm_out_ref, norm_sem)
    norm_copy.start()

    def out_copy(m):
        at = pl.ds(m * ROWS_OUT, ROWS_OUT)
        return pltpu.make_async_copy(stage.at[at], out_ref.at[at], sem.at[m])

    for m in range(n):
        at = pl.ds(m * ROWS_OUT, ROWS_OUT)
        stage[at, :] = jnp.where(keep, logits_ref[at, :] - norm, 0.0)
        out_copy(m).start()
    norm_copy.wait()
    for m in range(n):
        out_copy(m).wait()


def solution(mesh):
    def body(hidden_blk, end_pos, is_final, norm_gain, w_block):
        n_tok, hidden = hidden_blk.shape
        vocab = w_block.shape[1]
        n_req = end_pos.shape[0]
        n_slices = hidden // CW
        f32 = jnp.float32
        vmem = pl.BlockSpec(memory_space=pltpu.VMEM)
        hbm = pl.BlockSpec(memory_space=pl.ANY)
        dma = pltpu.SemaphoreType.DMA
        logits, norm = pl.pallas_call(
            gather_head_kernel,
            out_shape=(pltpu.VMEM((vocab, n_req), f32), pltpu.VMEM((1, n_req), f32)),
            in_specs=[hbm, hbm, hbm, hbm],
            out_specs=(vmem, vmem),
            scratch_shapes=[
                pltpu.VMEM((n_slices, 4 * n_tok, CW), jnp.bfloat16),
                pltpu.VMEM((W_SLOTS, vocab, WK), jnp.bfloat16),
                pltpu.VMEM((n_req, 4 * n_tok), jnp.bfloat16),
                pltpu.VMEM((2, n_req, WK), jnp.bfloat16),
                pltpu.VMEM((4, 8, n_tok), f32),
                pltpu.VMEM((4, 8, n_req), f32),
                pltpu.VMEM((1, n_req), jnp.int32),
                pltpu.VMEM((1, hidden), f32),
                dma((n_slices,)), dma((W_SLOTS, W_PIECES)), dma((2,)),
                dma((n_slices,)), dma((n_slices,)), dma((n_slices,)), dma((n_slices,)),
                dma((n_slices,)), dma((n_slices,)), dma((3,)), dma((3,)), dma((3,)), dma((3,)),
            ],
            compiler_params=pltpu.CompilerParams(
                collective_id=0, has_side_effects=True, vmem_limit_bytes=54 * 1024 * 1024
            ),
            name="gather_head",
        )(hidden_blk, end_pos.reshape(1, n_req), norm_gain.reshape(1, hidden), w_block.T)
        out, log_norm = pl.pallas_call(
            finish_kernel,
            out_shape=(jax.ShapeDtypeStruct((vocab, n_req), f32), jax.ShapeDtypeStruct((1, n_req), f32)),
            in_specs=[vmem, vmem, vmem],
            out_specs=(hbm, hbm),
            scratch_shapes=[pltpu.VMEM((vocab, n_req), f32), dma((vocab // ROWS_OUT,)), dma(())],
            compiler_params=pltpu.CompilerParams(vmem_limit_bytes=20 * 1024 * 1024),
            name="finish",
        )(logits, norm, is_final.reshape(1, n_req))
        return out.T, log_norm.reshape(n_req)

    return jax.shard_map(
        body,
        mesh=mesh,
        in_specs=(P(("dp", "tp"), None), P("dp"), P("dp"), P(None), P(None, "tp")),
        out_specs=(P("dp", "tp"), P("dp")),
        check_vma=False,
    )
```

```python
import jax
import jax.numpy as jnp
from jax import lax
from jax.experimental import pallas as pl
from jax.experimental.pallas import tpu as pltpu
from jax.sharding import PartitionSpec as P

NORM_EPS = 1e-5
MESH = pl.DeviceIdType.MESH
CW = 256
WK = 512
W_SLOTS = 5
W_PIECES = 4
ROWS_OUT = 1000
FIRST = 6400
LAST = 800


def gather_head_kernel(
    hidden_ref, pos_hbm, gain_hbm, w_ref, logits_ref, norm_ref,
    rows, w_ring, onehot, x_buf, inv_buf, stat_buf, pos_ref, gain_ref,
    own_sem, w_sem, in_sem, xs_sem, xr_sem, ps_sem, pr_sem, fs_sem, fr_sem, is_sem, ir_sem, ss_sem, sr_sem,
):
    n_tok, hidden = hidden_ref.shape
    vocab = w_ref.shape[0]
    n_req = pos_ref.shape[1]
    n_slices = hidden // CW
    n_w = hidden // WK
    per_w = WK // CW
    dp, me = lax.axis_index("dp"), lax.axis_index("tp")
    across = lax.rem(me + 2, 4)
    partner = me + 1 - 2 * lax.rem(me, 2)
    corner = lax.rem(partner + 2, 4)
    peers = (across, partner, corner)

    barrier = pltpu.get_barrier_semaphore()
    for peer in peers:
        pl.semaphore_signal(barrier, inc=1, device_id=(dp, peer), device_id_type=MESH)

    def block(owner):
        return pl.ds(pl.multiple_of(owner * n_tok, n_tok), n_tok)

    def own_copy(j):
        return pltpu.make_async_copy(
            hidden_ref.at[:, pl.ds(j * CW, CW)], rows.at[j, block(me)], own_sem.at[j]
        )

    def w_copy(s, p):
        m = vocab // W_PIECES
        return pltpu.make_async_copy(
            w_ref.at[pl.ds(p * m, m), pl.ds(s * WK, WK)],
            w_ring.at[s % W_SLOTS, pl.ds(p * m, m)],
            w_sem.at[s % W_SLOTS, p],
        )

    def send_rows(j, owner, send, recv, target):
        return pltpu.make_async_remote_copy(
            src_ref=rows.at[j, block(owner)], dst_ref=rows.at[j, block(owner)],
            send_sem=send.at[j], recv_sem=recv.at[j],
            device_id=(dp, target), device_id_type=MESH,
        )

    def to_across(j):
        return send_rows(j, me, xs_sem, xr_sem, across)

    def to_partner(j):
        return send_rows(j, me, ps_sem, pr_sem, partner)

    def forward(j):
        return send_rows(j, across, fs_sem, fr_sem, partner)

    def send_small(buf, i, send, recv):
        return pltpu.make_async_remote_copy(
            src_ref=buf.at[me], dst_ref=buf.at[me], send_sem=send.at[i], recv_sem=recv.at[i],
            device_id=(dp, peers[i]), device_id_type=MESH,
        )

    small = (
        pltpu.make_async_copy(pos_hbm, pos_ref, in_sem.at[0]),
        pltpu.make_async_copy(gain_hbm, gain_ref, in_sem.at[1]),
    )
    for j in range(n_slices):
        own_copy(j).start()
    for copy in small:
        copy.start()
    for s in range(min(W_SLOTS, n_w)):
        for p in range(W_PIECES):
            w_copy(s, p).start(priority=1)
    pl.semaphore_wait(barrier, 3)

    own_copy(0).wait()
    to_across(0).start()
    to_partner(0).start()
    for j in range(1, n_slices):
        own_copy(j).wait()
    total = jnp.zeros((n_tok, CW), jnp.float32)
    for j in range(n_slices):
        r = rows[j, block(me)].astype(jnp.float32)
        total += r * r
    inv = lax.rsqrt(jnp.sum(total, axis=1, keepdims=True) * (1.0 / hidden) + NORM_EPS)
    eye = lax.broadcasted_iota(jnp.int32, (n_tok, n_tok), 0) == lax.broadcasted_iota(jnp.int32, (n_tok, n_tok), 1)
    inv_row = jnp.sum(jnp.where(eye, inv, 0.0), axis=0, keepdims=True)
    inv_buf[me] = jnp.broadcast_to(inv_row, inv_buf.shape[1:])
    for j in range(1, n_slices):
        to_partner(j).start()
    for i in range(3):
        send_small(inv_buf, i, is_sem, ir_sem).start()
    for j in range(1, n_slices):
        to_across(j).start()
    for copy in small:
        copy.wait()
    picks = lax.broadcasted_iota(jnp.int32, (4 * n_tok, n_req), 0) == pos_ref[...]
    onehot[...] = jnp.where(picks, 1.0, 0.0).T.astype(jnp.bfloat16)

    def relay(j):
        to_across(j).wait_recv()
        forward(j).start()

    relay(0)
    for i in range(3):
        send_small(inv_buf, i, is_sem, ir_sem).wait_recv()
    inv_sel = jnp.zeros((n_req, 1), jnp.float32)
    for o in range(4):
        hit = onehot[:, o * n_tok:(o + 1) * n_tok].astype(jnp.float32)
        inv_sel += jnp.sum(hit * inv_buf[o, 0:1, :], axis=1, keepdims=True)

    def arrived(j):
        to_partner(j).wait_recv()
        forward(j).wait_recv()

    def prepare(j, k, slot):
        r = jnp.dot(onehot[...], rows[j], preferred_element_type=jnp.float32)
        x = r * inv_sel * gain_ref[:, j * CW:(j + 1) * CW]
        x_buf[slot, :, k * CW:(k + 1) * CW] = x.astype(jnp.bfloat16)

    steps = [tuple(range(s * per_w, (s + 1) * per_w)) for s in range(n_w)]
    once = 1 + me // 4

    def alone(work, *carry):
        return lax.fori_loop(0, once, lambda k, c: work(*c), carry)

    def multiply(i, start, size, lo=0, hi=WK):
        at = pl.ds(start, size)
        z = lax.dot_general(
            w_ring[i % W_SLOTS, at, lo:hi], x_buf[i % 2, :, lo:hi],
            (((1,), (1,)), ((), ())), preferred_element_type=jnp.float32,
        )
        if i > 0 or lo > 0:
            z += logits_ref[at, :]
        logits_ref[at, :] = z
        return z

    lanes = 4 * 8

    def highest(z, run_max):
        return jnp.maximum(run_max, jnp.max(z.reshape(z.shape[0] // lanes, lanes, n_req), axis=0))

    def w_wait(s):
        for p in range(W_PIECES):
            w_copy(s, p).wait()

    last = len(steps) - 1
    mid = vocab // 2

    def first_rows(i, mid=mid):
        prepare(steps[i][1], 1, i % 2)
        multiply(i, 0, mid, 0, CW)
        return multiply(i, 0, mid, CW, WK)

    def other_rows(i):
        prepare(steps[i + 1][0], 0, (i + 1) % 2)
        multiply(i, mid, vocab - mid)

    arrived(0)
    prepare(0, 0, 0)
    relay(1)
    w_wait(0)
    for i in range(last):
        nxt = steps[i + 1]
        arrived(steps[i][1])
        relay(nxt[0])
        alone(lambda: (first_rows(i), ())[1])
        relay(nxt[1])
        arrived(nxt[0])
        alone(lambda: (other_rows(i), ())[1])
        if i + W_SLOTS < n_w:
            for p in range(W_PIECES):
                w_copy(i + W_SLOTS, p).start(priority=1)
        w_wait(i + 1)
    arrived(steps[last][1])
    run_max = jnp.full((lanes, n_req), -jnp.inf, jnp.float32)

    def add_up(k, run_sum, top):
        z = logits_ref[pl.ds(pl.multiple_of(k * LAST, lanes), LAST), :]
        return run_sum + jnp.sum(jnp.exp(z.reshape(LAST // lanes, lanes, n_req) - top), axis=0)

    def second(ref):
        ref = highest(first_rows(last, FIRST), ref)
        run_max = highest(multiply(last, FIRST, vocab - FIRST), ref)
        run_sum = jnp.zeros((lanes, n_req), jnp.float32)
        for k in range(FIRST // LAST):
            run_sum = add_up(k, run_sum, ref)
        return run_max, run_sum * jnp.exp(ref - run_max)

    run_max, run_sum = lax.fori_loop(0, once, lambda k, c: second(c[0]), (run_max, run_max))
    run_sum = lax.fori_loop(FIRST // LAST, vocab // LAST, lambda k, c: add_up(k, c, run_max), run_sum)
    local_max = jnp.max(run_max, axis=0, keepdims=True)
    stat_buf[me, 0:1, :] = local_max
    stat_buf[me, 1:2, :] = jnp.sum(run_sum * jnp.exp(run_max - local_max), axis=0, keepdims=True)
    for i in range(3):
        send_small(stat_buf, i, ss_sem, sr_sem).start()
    for j in range(n_slices):
        to_across(j).wait_send()
        to_partner(j).wait_send()
        forward(j).wait_send()
    for i in range(3):
        send_small(inv_buf, i, is_sem, ir_sem).wait_send()
    for i in range(3):
        send_small(stat_buf, i, ss_sem, sr_sem).wait()
    group_max = jnp.max(stat_buf[:, 0, :], axis=0, keepdims=True)
    group_sum = jnp.sum(stat_buf[:, 1, :] * jnp.exp(stat_buf[:, 0, :] - group_max), axis=0, keepdims=True)
    norm_ref[...] = group_max + jnp.log(group_sum)


def finish_kernel(logits_ref, norm_ref, flag_ref, out_ref, norm_out_ref, stage, sem, norm_sem):
    vocab = logits_ref.shape[0]
    n = vocab // ROWS_OUT
    keep = flag_ref[...] == 1
    norm = norm_ref[...]
    norm_copy = pltpu.make_async_copy(norm_ref, norm_out_ref, norm_sem)
    norm_copy.start()

    def out_copy(m):
        at = pl.ds(m * ROWS_OUT, ROWS_OUT)
        return pltpu.make_async_copy(stage.at[at], out_ref.at[at], sem.at[m])

    for m in range(n):
        at = pl.ds(m * ROWS_OUT, ROWS_OUT)
        stage[at, :] = jnp.where(keep, logits_ref[at, :] - norm, 0.0)
        out_copy(m).start()
    norm_copy.wait()
    for m in range(n):
        out_copy(m).wait()


def solution(mesh):
    def body(hidden_blk, end_pos, is_final, norm_gain, w_block):
        n_tok, hidden = hidden_blk.shape
        vocab = w_block.shape[1]
        n_req = end_pos.shape[0]
        n_slices = hidden // CW
        f32 = jnp.float32
        vmem = pl.BlockSpec(memory_space=pltpu.VMEM)
        hbm = pl.BlockSpec(memory_space=pl.ANY)
        dma = pltpu.SemaphoreType.DMA
        logits, norm = pl.pallas_call(
            gather_head_kernel,
            out_shape=(pltpu.VMEM((vocab, n_req), f32), pltpu.VMEM((1, n_req), f32)),
            in_specs=[hbm, hbm, hbm, hbm],
            out_specs=(vmem, vmem),
            scratch_shapes=[
                pltpu.VMEM((n_slices, 4 * n_tok, CW), jnp.bfloat16),
                pltpu.VMEM((W_SLOTS, vocab, WK), jnp.bfloat16),
                pltpu.VMEM((n_req, 4 * n_tok), jnp.bfloat16),
                pltpu.VMEM((2, n_req, WK), jnp.bfloat16),
                pltpu.VMEM((4, 8, n_tok), f32),
                pltpu.VMEM((4, 8, n_req), f32),
                pltpu.VMEM((1, n_req), jnp.int32),
                pltpu.VMEM((1, hidden), f32),
                dma((n_slices,)), dma((W_SLOTS, W_PIECES)), dma((2,)),
                dma((n_slices,)), dma((n_slices,)), dma((n_slices,)), dma((n_slices,)),
                dma((n_slices,)), dma((n_slices,)), dma((3,)), dma((3,)), dma((3,)), dma((3,)),
            ],
            compiler_params=pltpu.CompilerParams(
                collective_id=0, has_side_effects=True, vmem_limit_bytes=54 * 1024 * 1024
            ),
            name="gather_head",
        )(hidden_blk, end_pos.reshape(1, n_req), norm_gain.reshape(1, hidden), w_block.T)
        out, log_norm = pl.pallas_call(
            finish_kernel,
            out_shape=(jax.ShapeDtypeStruct((vocab, n_req), f32), jax.ShapeDtypeStruct((1, n_req), f32)),
            in_specs=[vmem, vmem, vmem],
            out_specs=(hbm, hbm),
            scratch_shapes=[pltpu.VMEM((vocab, n_req), f32), dma((vocab // ROWS_OUT,)), dma(())],
            compiler_params=pltpu.CompilerParams(vmem_limit_bytes=20 * 1024 * 1024),
            name="finish",
        )(logits, norm, is_final.reshape(1, n_req))
        return out.T, log_norm.reshape(n_req)

    return jax.shard_map(
        body,
        mesh=mesh,
        in_specs=(P(("dp", "tp"), None), P("dp"), P("dp"), P(None), P(None, "tp")),
        out_specs=(P("dp", "tp"), P("dp")),
        check_vma=False,
    )
```
